32 devices in a mesh: group: 1, pool: 1, slab: 32 (over z, y, x, core).
Axes of the slice: x: 2, y: 2, z: 4, core: 2. Of those that a mesh axis runs over, the one named last changes fastest.
Arguments:
- drho_part: float32 [1, 16, 2, 128, 128, 128], P('pool', 'group', None, 'slab'), may hold values from -6 to 6
- fxc: float32 [128, 128, 128], P('slab'), may hold values from -2 to -0.2
- cutoff_mask: int32 [128, 128, 128], P(None, 'slab'), may hold values 0 or 1
- owner_table: int32 [16], P('group'), may hold values from 0 to 15, each once
Outputs:
- dv: float32 [16, 2, 128, 128, 128], P('group', None, 'slab')
The draws below stay inside these ranges and needn't reach their ends.
Inputs may be any that keep to these rules, and one draw needn't show every extreme that they name: `owner_table`: each perturbation appears in exactly one slot.
All inputs are finite; a program needn't handle non-finite values. No bound on the sum of `cutoff_mask` on one device may be relied on, other than what follows from the above.
Results may differ from the reference program's by a relative error of at most 0.00008.
Values sent between devices are 32-bit elements; how exact they have to be, the bound alone decides.
A program may use at most 128 MiB of HBM per device.

```python
import math
import jax
import jax.numpy as jnp
from jax import lax

NG = 128
P_SIZE = 16
N_POOL = 1


def set_ends(array, rng, smallest, top_value):
    longest = array.shape.index(max(array.shape))
    spots = []
    for shift in (0, 1):
        where = [jax.random.randint(jax.random.fold_in(rng, axis), (), 0, length) for axis, length in enumerate(array.shape)]
        where[longest] = (where[longest] + shift) % array.shape[longest]
        spots.append(tuple(where))
    return array.at[spots[0]].set(smallest).at[spots[1]].set(top_value)


def shard_levels(stream_key, extent, cuts, low, top_value):
    level, own = 1.0, jax.random.fold_in(stream_key, 6)
    for position, shards_of in cuts:
        steps = jnp.exp(jax.random.uniform(jax.random.fold_in(own, position), (shards_of,), jnp.float32, low / len(cuts), top_value / len(cuts)))
        level = level * jnp.repeat(steps, extent[position] // shards_of).reshape([-1 if axis == position else 1 for axis in range(len(extent))])
    return level


def gaussian(stream_key, extent, width, reach, pieces=(), kind=jnp.bfloat16):
    drawn = jax.random.normal(stream_key, extent, jnp.float32) * width
    if len(pieces) > 0:
        drawn = shard_levels(stream_key, extent, pieces, -0.22, 0.18) * drawn
    return jnp.clip(drawn, min=-reach, max=reach).astype(kind)


def setup_inputs(seed: int = 0, part: int = 0) -> dict:
    key_of = jax.random.split(jax.random.key(seed), 5)
    own_keys = jax.random.split(jax.random.fold_in(key_of[4], part), 5)
    drho_part = gaussian(own_keys[0], (N_POOL, P_SIZE, 2, NG, NG, NG), 1.0, 6.0, ((3, 32),), jnp.float32)
    fxc = jnp.clip(-2.0 + 1.8 * jax.random.uniform(key_of[1], (NG, NG, NG), jnp.float32) ** shard_levels(key_of[1], (NG, NG, NG), ((0, 32),), -0.2, 0.2), -2.0, -0.2)
    cutoff_mask = set_ends((jax.random.randint(key_of[2], (NG, NG, NG), 0, 4) < 3).astype(jnp.int32), jax.random.fold_in(key_of[2], 1), 0, 1)
    owner_table = jax.random.permutation(own_keys[3], P_SIZE).astype(jnp.int32)
    return dict(drho_part=drho_part, fxc=fxc, cutoff_mask=cutoff_mask, owner_table=owner_table)


def kernel_table(cutoff_mask):
    index = jnp.arange(NG, dtype=jnp.int32)
    freq = ((index + NG // 2) % NG - NG // 2).astype(jnp.float32)
    square = freq * freq
    total = square[:, None, None] + square[None, :, None] + square[None, None, :]
    unit = (2.0 * math.pi / NG) ** 2
    return 4.0 * math.pi * cutoff_mask.astype(jnp.float32) / (unit * total + 0.25)


def reference(drho_part, fxc, cutoff_mask, owner_table):
    density = jnp.sum(drho_part, axis=0)
    ordered = jnp.take(density, owner_table, axis=0)
    kernel = kernel_table(cutoff_mask)

    def single(field):
        spectrum = jnp.fft.fftn(lax.complex(field[0], field[1]))
        hartree = jnp.fft.ifftn(spectrum * kernel)
        return jnp.stack([jnp.real(hartree) + fxc * field[0], jnp.imag(hartree) + fxc * field[1]])

    return lax.map(single, ordered)
```

```python
import functools
import math

import jax
import jax.numpy as jnp
import numpy as np
from jax import lax
from jax.experimental import pallas as pl
from jax.experimental.pallas import tpu as pltpu
from jax.sharding import PartitionSpec as P

CHUNKS = 2
VMEM_MIB = 60


def halves(matrix):
    high = matrix.astype(np.float32).astype(jnp.bfloat16)
    low = (matrix - high.astype(np.float64)).astype(np.float32).astype(jnp.bfloat16)
    return np.stack([high, low])


def complex_dft(length, sign):
    index = np.arange(length)
    angle = (index[:, None] * index[None, :] % length) * (2.0 * math.pi / length)
    cosine, sine = np.cos(angle), sign * np.sin(angle)
    return np.block([[cosine, -sine], [sine, cosine]])


def slab_order(length, width):
    table = np.arange(2 * length).reshape(2, length // width, width)
    return table.transpose(1, 0, 2).reshape(-1)


def inner_order(length, width):
    table = np.arange(2 * length).reshape(2, length // width, width)
    return table.transpose(2, 0, 1).reshape(-1)


def split(value):
    high = value.astype(jnp.bfloat16)
    low = (value - high.astype(jnp.float32)).astype(jnp.bfloat16)
    return high, low


def dot(left, right):
    return jnp.dot(left, right, preferred_element_type=jnp.float32)


def left_dot(matrix_ref, value):
    high, low = split(value)
    return dot(matrix_ref[0], high) + (dot(matrix_ref[1], high) + dot(matrix_ref[0], low))


def right_dot(value, matrix_ref):
    high, low = split(value)
    return dot(high, matrix_ref[0]) + (dot(low, matrix_ref[0]) + dot(high, matrix_ref[1]))


def forward_kernel(owner_ref, field_ref, along_z_ref, along_y_ref, out_ref):
    _, _, width, length, _ = field_ref.shape
    slabs = length // width
    rows = width * length
    field = jnp.concatenate(
        [field_ref[0, 0].reshape(rows, length), field_ref[0, 1].reshape(rows, length)], axis=1
    )
    field = right_dot(field, along_z_ref)
    field = jnp.concatenate(
        [
            jnp.concatenate(
                [field[x * length : (x + 1) * length, c * length : (c + 1) * length] for c in range(2)], axis=0
            )
            for x in range(width)
        ],
        axis=1,
    )
    field = left_dot(along_y_ref, field)
    for y in range(width):
        for c in range(2):
            first = (y * 2 + c) * slabs
            for x in range(width):
                out_ref[:, 0, c * width + x, y * length : (y + 1) * length] = field[
                    first : first + slabs, x * length : (x + 1) * length
                ]


def column_stage(field_ref, screen_ref, forth_ref, back_ref, out_ref):
    slabs, _, rows, lanes = field_ref.shape
    length = screen_ref.shape[0]
    field = field_ref[:, 0].reshape(slabs * rows, lanes)
    field = left_dot(forth_ref, field)
    screen = screen_ref[...]
    field = jnp.concatenate([field[:length] * screen, field[length:] * screen], axis=0)
    field = left_dot(back_ref, field)
    out_ref[:, 0] = field.reshape(slabs, rows, lanes)


def backward_kernel(owner_ref, field_ref, density_ref, fxc_ref, along_y_ref, along_z_ref, *rest):
    out_ref = rest[-1]
    _, _, width, length, _ = density_ref.shape
    field = jnp.concatenate(
        [
            jnp.concatenate(
                [
                    field_ref[:, 0, c * width + x, y * length : (y + 1) * length]
                    for y in range(width)
                    for c in range(2)
                ],
                axis=0,
            )
            for x in range(width)
        ],
        axis=1,
    )
    field = left_dot(along_y_ref, field)
    field = jnp.concatenate(
        [
            jnp.concatenate(
                [field[c * length : (c + 1) * length, x * length : (x + 1) * length] for c in range(2)], axis=1
            )
            for x in range(width)
        ],
        axis=0,
    )
    field = right_dot(field, along_z_ref)
    fxc = fxc_ref[...]
    for c in range(2):
        part = field[:, c * length : (c + 1) * length].reshape(width, length, length)
        out_ref[0, c] = part + fxc * density_ref[0, c]


def frequency(index, length):
    return ((index + length // 2) % length - length // 2).astype(jnp.float32)


def column_screen(cutoff_mask, length):
    width = cutoff_mask.shape[1]
    start = lax.axis_index("slab") * width
    full_index = jnp.arange(length, dtype=jnp.int32)
    part_index = start + jnp.arange(width, dtype=jnp.int32)
    full_square = frequency(full_index, length) ** 2
    part_square = frequency(part_index, length) ** 2
    total = full_square[:, None, None] + part_square[None, :, None] + full_square[None, None, :]
    unit = (2.0 * math.pi / length) ** 2
    screen = 4.0 * math.pi * cutoff_mask.astype(jnp.float32) / (unit * total + 0.25)
    return (screen * (1.0 / float(length**3))).reshape(length, width * length)


def whole_spec(array):
    zeros = (0,) * array.ndim
    return pl.BlockSpec(array.shape, lambda *_: zeros)


def cost(count, rows, length):
    size = 2 * rows * length
    return pl.CostEstimate(flops=count * 24 * size * length, bytes_accessed=count * 8 * size, transcendentals=0)


def per_device(drho_part, fxc, cutoff_mask, owner_table):
    density = drho_part[0]
    if lax.axis_size("pool") > 1:
        density = lax.psum(density, "pool")
    count, _, width, length, _ = density.shape
    slabs = length // width
    rows, lanes = 2 * width, width * length
    chunks = math.gcd(CHUNKS, count)
    each = count // chunks

    forth, back = complex_dft(length, -1.0), complex_dft(length, 1.0)
    by_slab, by_inner = slab_order(length, width), inner_order(length, width)
    z_forth, z_back = jnp.asarray(halves(forth.T)), jnp.asarray(halves(back.T))
    y_forth, y_back = jnp.asarray(halves(forth[by_inner])), jnp.asarray(halves(back[:, by_inner]))
    x_forth, x_back = jnp.asarray(halves(forth[:, by_slab])), jnp.asarray(halves(back[by_slab]))
    screen = column_screen(cutoff_mask, length)

    params = pltpu.CompilerParams(dimension_semantics=("arbitrary",), vmem_limit_bytes=VMEM_MIB * 2**20)
    packed = jax.ShapeDtypeStruct((slabs, each, rows, lanes), jnp.float32)
    packed_spec = pl.BlockSpec((slabs, 1, rows, lanes), lambda i, *_: (0, i, 0, 0))
    price = cost(each, lanes, length)

    def forward(chunk):
        return pl.pallas_call(
            forward_kernel,
            out_shape=packed,
            grid_spec=pltpu.PrefetchScalarGridSpec(
                num_scalar_prefetch=1,
                grid=(each,),
                in_specs=[
                    pl.BlockSpec(
                        (1, 2, width, length, length), lambda i, owner: (owner[chunk * each + i], 0, 0, 0, 0)
                    ),
                    whole_spec(z_forth),
                    whole_spec(y_forth),
                ],
                out_specs=packed_spec,
            ),
            compiler_params=params,
            cost_estimate=price,
        )(owner_table, density, z_forth, y_forth)

    def columns(field):
        return pl.pallas_call(
            column_stage,
            out_shape=packed,
            grid=(each,),
            in_specs=[packed_spec, whole_spec(screen), whole_spec(x_forth), whole_spec(x_back)],
            out_specs=packed_spec,
            compiler_params=params,
            cost_estimate=price,
        )(field, screen, x_forth, x_back)

    def backward(chunk, field, result):
        earlier = [] if result is None else [result]
        return pl.pallas_call(
            backward_kernel,
            out_shape=jax.ShapeDtypeStruct(density.shape, jnp.float32),
            grid_spec=pltpu.PrefetchScalarGridSpec(
                num_scalar_prefetch=1,
                grid=(each,),
                in_specs=[
                    packed_spec,
                    pl.BlockSpec(
                        (1, 2, width, length, length), lambda i, owner: (owner[chunk * each + i], 0, 0, 0, 0)
                    ),
                    whole_spec(fxc),
                    whole_spec(y_back),
                    whole_spec(z_back),
                ]
                + [pl.BlockSpec(memory_space=pl.ANY)] * len(earlier),
                out_specs=pl.BlockSpec(
                    (1, 2, width, length, length), lambda i, owner: (chunk * each + i, 0, 0, 0, 0)
                ),
            ),
            input_output_aliases={6: 0} if earlier else {},
            compiler_params=params,
            cost_estimate=price,
        )(owner_table, field, density, fxc, y_back, z_back, *earlier)

    def swap(field):
        return lax.all_to_all(field, "slab", split_axis=0, concat_axis=0, tiled=True)

    spectra = [swap(forward(chunk)) for chunk in range(chunks)]
    spectra = [swap(columns(field)) for field in spectra]
    result = None
    for chunk, field in enumerate(spectra):
        result = backward(chunk, field, result)
    return result


def solution(mesh):
    placed = (
        P("pool", "group", None, "slab", None, None),
        P("slab", None, None),
        P(None, "slab", None),
        P("group"),
    )
    return jax.shard_map(
        per_device,
        mesh=mesh,
        in_specs=placed,
        out_specs=P("group", None, "slab", None, None),
        check_vma=False,
    )
```

```python
import functools
import math

import jax
import jax.numpy as jnp
import numpy as np
from jax import lax
from jax.experimental import pallas as pl
from jax.experimental.pallas import tpu as pltpu
from jax.sharding import PartitionSpec as P

CHUNKS = 2
VMEM_MIB = 60
PER_STEP = 2


def halves(matrix):
    high = matrix.astype(np.float32).astype(jnp.bfloat16)
    low = (matrix - high.astype(np.float64)).astype(np.float32).astype(jnp.bfloat16)
    return np.stack([high, low])


def complex_dft(length, sign):
    index = np.arange(length)
    angle = (index[:, None] * index[None, :] % length) * (2.0 * math.pi / length)
    cosine, sine = np.cos(angle), sign * np.sin(angle)
    return np.block([[cosine, -sine], [sine, cosine]])


def slab_order(length, width):
    table = np.arange(2 * length).reshape(2, length // width, width)
    return table.transpose(1, 0, 2).reshape(-1)


def inner_order(length, width):
    table = np.arange(2 * length).reshape(2, length // width, width)
    return table.transpose(2, 0, 1).reshape(-1)


def split(value):
    high = value.astype(jnp.bfloat16)
    low = (value - high.astype(jnp.float32)).astype(jnp.bfloat16)
    return high, low


def dot(left, right):
    return jnp.dot(left, right, preferred_element_type=jnp.float32)


def left_dot(matrix_ref, value):
    high, low = split(value)
    return dot(matrix_ref[0], high) + (dot(matrix_ref[1], high) + dot(matrix_ref[0], low))


def right_dot(value, matrix_ref):
    high, low = split(value)
    return dot(high, matrix_ref[0]) + (dot(low, matrix_ref[0]) + dot(high, matrix_ref[1]))


def forward_kernel(owner_ref, *refs):
    *field_refs, along_z_ref, along_y_ref, out_ref = refs
    _, _, width, length, _ = field_refs[0].shape
    slabs = length // width
    rows = width * length
    fields = [
        jnp.concatenate([ref[0, 0].reshape(rows, length), ref[0, 1].reshape(rows, length)], axis=1)
        for ref in field_refs
    ]
    fields = [right_dot(field, along_z_ref) for field in fields]
    fields = [
        jnp.concatenate(
            [
                jnp.concatenate(
                    [field[x * length : (x + 1) * length, c * length : (c + 1) * length] for c in range(2)], axis=0
                )
                for x in range(width)
            ],
            axis=1,
        )
        for field in fields
    ]
    fields = [left_dot(along_y_ref, field) for field in fields]
    for slot, field in enumerate(fields):
        for y in range(width):
            for c in range(2):
                first = (y * 2 + c) * slabs
                for x in range(width):
                    out_ref[:, slot, c * width + x, y * length : (y + 1) * length] = field[
                        first : first + slabs, x * length : (x + 1) * length
                    ]


def column_stage(field_ref, screen_ref, forth_ref, back_ref, out_ref):
    slabs, slots, rows, lanes = field_ref.shape
    length = screen_ref.shape[0]
    fields = [field_ref[:, slot].reshape(slabs * rows, lanes) for slot in range(slots)]
    fields = [left_dot(forth_ref, field) for field in fields]
    screen = screen_ref[...]
    fields = [jnp.concatenate([field[:length] * screen, field[length:] * screen], axis=0) for field in fields]
    fields = [left_dot(back_ref, field) for field in fields]
    for slot, field in enumerate(fields):
        out_ref[:, slot] = field.reshape(slabs, rows, lanes)


def backward_kernel(slots, owner_ref, field_ref, *refs):
    density_refs, out_ref = refs[:slots], refs[-1]
    fxc_ref, along_y_ref, along_z_ref = refs[slots : slots + 3]
    _, _, width, length, _ = density_refs[0].shape
    fields = [
        jnp.concatenate(
            [
                jnp.concatenate(
                    [
                        field_ref[:, slot, c * width + x, y * length : (y + 1) * length]
                        for y in range(width)
                        for c in range(2)
                    ],
                    axis=0,
                )
                for x in range(width)
            ],
            axis=1,
        )
        for slot in range(slots)
    ]
    fields = [left_dot(along_y_ref, field) for field in fields]
    fields = [
        jnp.concatenate(
            [
                jnp.concatenate(
                    [field[c * length : (c + 1) * length, x * length : (x + 1) * length] for c in range(2)], axis=1
                )
                for x in range(width)
            ],
            axis=0,
        )
        for field in fields
    ]
    fields = [right_dot(field, along_z_ref) for field in fields]
    fxc = fxc_ref[...]
    for slot, field in enumerate(fields):
        for c in range(2):
            part = field[:, c * length : (c + 1) * length].reshape(width, length, length)
            out_ref[slot, c] = part + fxc * density_refs[slot][0, c]


def frequency(index, length):
    return ((index + length // 2) % length - length // 2).astype(jnp.float32)


def column_screen(cutoff_mask, length):
    width = cutoff_mask.shape[1]
    start = lax.axis_index("slab") * width
    full_index = jnp.arange(length, dtype=jnp.int32)
    part_index = start + jnp.arange(width, dtype=jnp.int32)
    full_square = frequency(full_index, length) ** 2
    part_square = frequency(part_index, length) ** 2
    total = full_square[:, None, None] + part_square[None, :, None] + full_square[None, None, :]
    unit = (2.0 * math.pi / length) ** 2
    screen = 4.0 * math.pi * cutoff_mask.astype(jnp.float32) / (unit * total + 0.25)
    return (screen * (1.0 / float(length**3))).reshape(length, width * length)


def whole_spec(array):
    zeros = (0,) * array.ndim
    return pl.BlockSpec(array.shape, lambda *_: zeros)


def cost(count, rows, length):
    size = 2 * rows * length
    return pl.CostEstimate(flops=count * 24 * size * length, bytes_accessed=count * 8 * size, transcendentals=0)


def per_device(drho_part, fxc, cutoff_mask, owner_table):
    density = drho_part[0]
    if lax.axis_size("pool") > 1:
        density = lax.psum(density, "pool")
    count, _, width, length, _ = density.shape
    slabs = length // width
    rows, lanes = 2 * width, width * length
    chunks = math.gcd(CHUNKS, count)
    each = count // chunks
    slots = math.gcd(PER_STEP, each)
    steps = each // slots

    forth, back = complex_dft(length, -1.0), complex_dft(length, 1.0)
    by_slab, by_inner = slab_order(length, width), inner_order(length, width)
    z_forth, z_back = jnp.asarray(halves(forth.T)), jnp.asarray(halves(back.T))
    y_forth, y_back = jnp.asarray(halves(forth[by_inner])), jnp.asarray(halves(back[:, by_inner]))
    x_forth, x_back = jnp.asarray(halves(forth[:, by_slab])), jnp.asarray(halves(back[by_slab]))
    screen = column_screen(cutoff_mask, length)

    params = pltpu.CompilerParams(dimension_semantics=("arbitrary",), vmem_limit_bytes=VMEM_MIB * 2**20)
    packed = jax.ShapeDtypeStruct((slabs, each, rows, lanes), jnp.float32)
    packed_spec = pl.BlockSpec((slabs, slots, rows, lanes), lambda i, *_: (0, i, 0, 0))
    price = cost(each, lanes, length)

    def owned(chunk, slot):
        return pl.BlockSpec(
            (1, 2, width, length, length), lambda i, owner: (owner[chunk * each + i * slots + slot], 0, 0, 0, 0)
        )

    def forward(chunk):
        return pl.pallas_call(
            forward_kernel,
            out_shape=packed,
            grid_spec=pltpu.PrefetchScalarGridSpec(
                num_scalar_prefetch=1,
                grid=(steps,),
                in_specs=[owned(chunk, slot) for slot in range(slots)]
                + [
                    whole_spec(z_forth),
                    whole_spec(y_forth),
                ],
                out_specs=packed_spec,
            ),
            compiler_params=params,
            cost_estimate=price,
        )(owner_table, *[density] * slots, z_forth, y_forth)

    def columns(field):
        return pl.pallas_call(
            column_stage,
            out_shape=packed,
            grid=(steps,),
            in_specs=[packed_spec, whole_spec(screen), whole_spec(x_forth), whole_spec(x_back)],
            out_specs=packed_spec,
            compiler_params=params,
            cost_estimate=price,
        )(field, screen, x_forth, x_back)

    def backward(chunk, field, result):
        earlier = [] if result is None else [result]
        return pl.pallas_call(
            functools.partial(backward_kernel, slots),
            out_shape=jax.ShapeDtypeStruct(density.shape, jnp.float32),
            grid_spec=pltpu.PrefetchScalarGridSpec(
                num_scalar_prefetch=1,
                grid=(steps,),
                in_specs=[packed_spec]
                + [owned(chunk, slot) for slot in range(slots)]
                + [
                    whole_spec(fxc),
                    whole_spec(y_back),
                    whole_spec(z_back),
                ]
                + [pl.BlockSpec(memory_space=pl.ANY)] * len(earlier),
                out_specs=pl.BlockSpec(
                    (slots, 2, width, length, length), lambda i, owner: (chunk * steps + i, 0, 0, 0, 0)
                ),
            ),
            input_output_aliases={5 + slots: 0} if earlier else {},
            compiler_params=params,
            cost_estimate=price,
        )(owner_table, field, *[density] * slots, fxc, y_back, z_back, *earlier)

    def swap(field):
        return lax.all_to_all(field, "slab", split_axis=0, concat_axis=0, tiled=True)

    spectra = [swap(forward(chunk)) for chunk in range(chunks)]
    spectra = [swap(columns(field)) for field in spectra]
    result = None
    for chunk, field in enumerate(spectra):
        result = backward(chunk, field, result)
    return result


def solution(mesh):
    placed = (
        P("pool", "group", None, "slab", None, None),
        P("slab", None, None),
        P(None, "slab", None),
        P("group"),
    )
    return jax.shard_map(
        per_device,
        mesh=mesh,
        in_specs=placed,
        out_specs=P("group", None, "slab", None, None),
        check_vma=False,
    )
```
